32 devices in a mesh: section: 4 (over y, x), scen: 8 (over z, core).
Axes of the slice: x: 2, y: 2, z: 4, core: 2. Of those that a mesh axis runs over, the one named last changes fastest.
Arguments:
- scenario_data: bfloat16 [512, 3, 4, 4096], P(('scen', 'section')), may hold values from -6 to 6
- cost_matrix: bfloat16 [4096, 4096], P('section'), may hold values from -0.09375 to 0.09375
- curvature: bfloat16 [512, 3, 4, 4096], P(('scen', 'section')), may hold values from 0.25 to 4
- upper: bfloat16 [512, 3, 4, 4096], P(('scen', 'section')), may hold values from 0.1 to 14
- multipliers: float32 [512, 2, 4, 4096], P(('scen', 'section')), may hold values from -4 to 4
- node_map: int32 [8, 64], P('scen'), may hold values from 0 to 7, never falling along the last dimension, each value on 1 to 16 neighbouring positions
Outputs:
- new_multipliers: float32 [512, 2, 4, 4096], P(('scen', 'section'))
- decisions: float32 [512, 3, 4, 4096], P(('scen', 'section'))
The draws below stay inside these ranges and needn't reach their ends.
Inputs may be any that keep to these rules, and one draw needn't show every extreme that they name: node_map[g, k] is the second-level node of scenario g * 64 + k; every node of a group has at least one scenario.
All inputs are finite; a program needn't handle non-finite values.
Results may differ from the reference program's by a relative error of at most 0.0003.
Values may be sent and summed in bfloat16 or wider, within the bound.
No kernel may reach another device: no remote copies, remote signals or barrier semaphores. Data moves between devices by JAX's collectives and lax.ppermute only.
A program may use at most 128 MiB of HBM per device.

```python
import math
import jax
import jax.numpy as jnp
import numpy as np
from jax import lax

W = 4096
PER = 4
NODES_GRP = 8
MOST = 16
GROUP = 64
GROUPS = 8
SCENARIOS = 512


def draw_upper(key, part):
    ramp = 3.0 ** (jnp.arange(SCENARIOS, dtype=jnp.float32) / (SCENARIOS - 1))
    base = jax.random.uniform(key, (SCENARIOS, 3, PER, W), jnp.float32, 0.2, 1.2)
    value = base * ramp[:, None, None, None]
    return value.astype(jnp.bfloat16)


def steps_of(stream_key, extent, pieces, low, largest):
    level, own = 1.0, jax.random.fold_in(stream_key, 6)
    for position, shards_of in pieces:
        heights = jnp.exp(jax.random.uniform(jax.random.fold_in(own, position), (shards_of,), jnp.float32, low / len(pieces), largest / len(pieces)))
        level = level * jnp.repeat(heights, extent[position] // shards_of).reshape([-1 if axis == position else 1 for axis in range(len(extent))])
    return level


def profile(amount, total, most, lean):
    portions = [(1 << 20) // math.isqrt(grade ** lean) + 1 for grade in range(2, amount + 1)]
    rest, given = total - most - (amount - 1), [1] * (amount - 1)
    while rest > 0:
        movable = [i for i in range(amount - 1) if given[i] < most]
        pool, remaining = sum([portions[i] for i in movable]), rest
        for i in movable:
            addition = min(most - given[i], max(1, remaining * portions[i] // pool), rest)
            given[i] = given[i] + addition
            rest = rest - addition
    return np.array([most] + given)


def ragged(stream_key, number_of, total, reach, slope):
    if number_of == 2:
        one = jax.random.randint(stream_key, (), max(1, total - reach), min(reach, total - 1) + 1)
        return jnp.stack([one, total - one])
    lengths = jnp.asarray(profile(number_of, total, reach, slope), jnp.int32)
    pairs = (number_of - 1) // 2
    donor, receiver = lengths[1:1 + 2 * pairs:2], lengths[2:2 + 2 * pairs:2]
    margin = jnp.minimum(donor - 1, reach - receiver)
    passed = jax.random.randint(jax.random.fold_in(stream_key, 1), (pairs,), 0, 1 << 20) % (margin + 1)
    lengths = lengths.at[1:1 + 2 * pairs:2].set(donor - passed).at[2:2 + 2 * pairs:2].set(receiver + passed)
    return lengths[jax.random.permutation(jax.random.fold_in(stream_key, 2), number_of)]


def noise(stream_key, dims, scale, limit, shards=(), held_as=jnp.bfloat16):
    result = jax.random.normal(stream_key, dims, jnp.float32) * scale
    if len(shards) > 0:
        result = steps_of(stream_key, dims, shards, -0.22, 0.18) * result
    return jnp.clip(result, min=-limit, max=limit).astype(held_as)


def setup_inputs(seed: int = 0) -> dict:
    key_list = jax.random.split(jax.random.key(seed), 7)
    return {
        "scenario_data": noise(key_list[0], (SCENARIOS, 3, PER, W), 1.0, 6.0, ((0, 32),)),
        "cost_matrix": noise(key_list[1], (W, W), W ** -0.5, 0.09375, ((0, 4),)),
        "curvature": jnp.clip(jnp.exp(math.log(4.0) - 2.7725887 * jax.random.uniform(key_list[2], (SCENARIOS, 3, PER, W), jnp.float32) ** steps_of(key_list[2], (SCENARIOS, 3, PER, W), ((0, 32),), -0.2, 0.2)), 0.25, 4.0).astype(jnp.bfloat16),
        "upper": draw_upper(jax.random.fold_in(key_list[6], 71), 0),
        "multipliers": noise(key_list[4], (SCENARIOS, 2, PER, W), 0.5, 4.0, ((0, 32),), jnp.float32),
        "node_map": jax.vmap(lambda own: jnp.searchsorted(jnp.cumsum(ragged(own, NODES_GRP, GROUP, MOST, 1)), jnp.arange(GROUP), side="right"))(jax.random.split(key_list[5], GROUPS)).reshape((GROUPS, GROUP)).astype(jnp.int32),
    }


def reference(scenario_data, cost_matrix, curvature, upper, multipliers, node_map):
    scenarios = scenario_data.shape[0]
    rows = scenario_data.reshape(scenarios * 3 * PER, W)
    cost = jnp.dot(rows, cost_matrix.T, preferred_element_type=jnp.float32).reshape(scenarios, 3, PER, W)
    padding = jnp.zeros((scenarios, 1, PER, W), jnp.float32)
    linear = cost + jnp.concatenate([multipliers, padding], axis=1)
    decisions = jnp.clip(-linear / curvature.astype(jnp.float32), 0.0, upper.astype(jnp.float32))
    first = decisions[:, 0]
    root_mean = lax.optimization_barrier(jnp.sum(first, axis=0)) / scenarios
    groups = node_map.shape[0]
    second = decisions[:, 1].reshape(groups, GROUP, PER * W)
    labels = jnp.arange(NODES_GRP, dtype=jnp.int32)
    member = (node_map[:, None, :] == labels[None, :, None]).astype(jnp.float32)
    counts = lax.optimization_barrier(jnp.sum(member, axis=2))
    node_total = jnp.einsum('gns,gsf->gnf', member, second, precision=lax.Precision.HIGHEST)
    node_mean = node_total / counts[:, :, None]
    back = jnp.einsum('gns,gnf->gsf', member, node_mean, precision=lax.Precision.HIGHEST)
    first_gap = first - root_mean[None]
    second_gap = (second - back).reshape(scenarios, PER, W)
    spread = jnp.sum(first_gap * first_gap) + jnp.sum(second_gap * second_gap)
    step = 0.5 / jnp.sqrt(spread / (2.0 * scenarios * PER * W) + 1e-06)
    gap = jnp.stack([first_gap, second_gap], axis=1)
    return (multipliers + step * gap, decisions)
```

```python
import functools
import math

import jax
import jax.numpy as jnp
from jax import lax
from jax.experimental import pallas as pl
from jax.experimental.pallas import tpu as pltpu
from jax.sharding import PartitionSpec as P

ENTRY_BOUND = 6.0 * 0.09375
KNEE = 0.25
CODES = 32767.0
F32 = jnp.float32
LANES = 128


def code_scale(width):
    return CODES / math.asinh(1.0001 * width * ENTRY_BOUND / KNEE)


def encode(cost, scale):
    size = jnp.abs(cost) * (1.0 / KNEE)
    code = jnp.log(size + jnp.sqrt(size * size + 1.0)) * scale + 0.5
    code = code.astype(jnp.int32)
    return jnp.where(cost < 0, -code, code).astype(jnp.int16)


def decode(code, scale):
    grown = jnp.exp(code.astype(F32) * (1.0 / scale))
    return (0.5 * KNEE) * (grown - 1.0 / grown)


def xor_permute(value, axis, mask):
    count = lax.axis_size(axis)
    return lax.ppermute(value, axis, [(i, i ^ mask) for i in range(count)])


def matmul(pieces, cost_matrix, outs, scale=None, cols=256):
    rows = sum(piece.shape[0] for piece in pieces)
    height, width = cost_matrix.shape
    out_rows = rows // outs
    dtype = F32 if scale is None else jnp.int16

    def kernel(*refs):
        xs = refs[: len(pieces)]
        matrix = refs[len(pieces)]
        results = refs[len(pieces) + 1 : len(pieces) + 1 + outs]
        stacked = refs[-1]

        @pl.when(pl.program_id(0) == 0)
        def _():
            at = 0
            for x in xs:
                stacked[at : at + x.shape[0], :] = x[...]
                at += x.shape[0]

        acc = lax.dot_general(stacked[...], matrix[...], (((1,), (1,)), ((), ())), preferred_element_type=F32)
        if scale is not None:
            acc = encode(acc, scale)
        for i, result in enumerate(results):
            result[...] = acc[i * out_rows : (i + 1) * out_rows]

    return pl.pallas_call(
        kernel,
        grid=(height // cols,),
        in_specs=[pl.BlockSpec(p.shape, lambda i: (0, 0)) for p in pieces] + [pl.BlockSpec((cols, width), lambda i: (i, 0))],
        out_specs=[pl.BlockSpec((out_rows, cols), lambda i: (0, i))] * outs,
        out_shape=[jax.ShapeDtypeStruct((out_rows, height), dtype)] * outs,
        scratch_shapes=[pltpu.VMEM((rows, width), jnp.bfloat16)],
        cost_estimate=pl.CostEstimate(flops=2 * rows * height * width, bytes_accessed=2 * (rows + height) * width, transcendentals=0),
    )(*pieces, cost_matrix)


def decide(level, section, own, coded, curvature, upper, multipliers, decisions, scale, extra=None, extra_specs=(), extra_shapes=(), extra_args=(), keep=True):
    sc_dev, levels, periods, width = curvature.shape
    block = own.shape[1]
    has_mult = level < multipliers.shape[1]
    group = 16 // periods
    n_fixed = 4 + len(coded) + (1 if has_mult else 0) + (1 if decisions is not None else 0)

    def kernel(*refs):
        refs = list(refs)
        sec = refs.pop(0)[0]
        own_ref = refs.pop(0)
        coded_refs = [refs.pop(0) for _ in coded]
        cur, upp = refs.pop(0), refs.pop(0)
        mul = refs.pop(0) if has_mult else None
        if decisions is not None:
            refs.pop(0)
        extra_in = [refs.pop(0) for _ in extra_args]
        out = refs.pop(0)
        kept = refs.pop(0) if keep else None
        for k, ref in enumerate([own_ref] + coded_refs):
            col = pl.ds(pl.multiple_of((sec ^ k) * block, LANES), block)
            for a in range(sc_dev // group):
                mine = slice(group * a, group * (a + 1))
                cost = ref[16 * a : 16 * (a + 1), :]
                if k > 0:
                    cost = decode(cost, scale)
                linear = cost.reshape(group, periods, block)
                if has_mult:
                    linear = linear + mul[mine, 0, :, col]
                value = jnp.clip(-linear / cur[mine, 0, :, col].astype(F32), 0.0, upp[mine, 0, :, col].astype(F32))
                out[mine, 0, :, col] = value
                if keep:
                    kept[mine, :, col] = value
        if extra is not None:
            extra(kept, extra_in, refs)

    at_level = lambda i: (0, level, 0, 0)
    fixed = lambda i: (0, 0)
    big = pl.BlockSpec((sc_dev, 1, periods, width), at_level)
    in_specs = [pl.BlockSpec(memory_space=pltpu.SMEM)] + [pl.BlockSpec(own.shape, fixed)] * (1 + len(coded)) + [big, big]
    args = [section, own, *coded, curvature, upper]
    if has_mult:
        in_specs.append(big)
        args.append(multipliers)
    aliases = {}
    if decisions is not None:
        aliases[len(args)] = 0
        in_specs.append(pl.BlockSpec(memory_space=pl.ANY))
        args.append(decisions)
    in_specs += [spec for spec, _ in extra_args]
    args += [value for _, value in extra_args]
    out_specs = [big]
    out_shape = [jax.ShapeDtypeStruct(curvature.shape, F32)]
    if keep:
        out_specs.append(pl.BlockSpec((sc_dev, periods, width), lambda i: (0, 0, 0)))
        out_shape.append(jax.ShapeDtypeStruct((sc_dev, periods, width), F32))
    return pl.pallas_call(
        kernel,
        grid=(1,),
        in_specs=in_specs,
        out_specs=out_specs + list(extra_specs),
        out_shape=out_shape + list(extra_shapes),
        input_output_aliases=aliases,
        cost_estimate=pl.CostEstimate(flops=4000000, bytes_accessed=4000000, transcendentals=0),
    )(*args)


def lane_sum(squares):
    total = squares[:, :LANES]
    for j in range(1, squares.shape[1] // LANES):
        total = total + squares[:, j * LANES : (j + 1) * LANES]
    return total


def combine(messages, count):
    periods, length = messages[0].shape
    width = length - LANES

    def kernel(*refs):
        *ins, out = refs
        total = ins[0][...]
        for ref in ins[1:]:
            total = total + ref[...]
        mean = total[:, :width] * (1.0 / len(ins))
        squares = jnp.zeros((periods, width), F32)
        for ref in ins:
            off = ref[:, :width] - mean
            squares = squares + off * off
        out[:, :width] = total[:, :width]
        out[:, width:] = total[:, width:] + lane_sum(squares) * (1.0 / count)

    return pl.pallas_call(kernel, out_shape=jax.ShapeDtypeStruct((periods, length), F32))(*messages)


def root_reduce(message, count):
    stages = []
    for axis, first in (("scen", 1), ("section", 0)):
        bits = lax.axis_size(axis).bit_length() - 1
        if first:
            stages.append((axis, [1]))
        at = first
        while at < bits:
            if at + 1 < bits:
                stages.append((axis, [1 << at, 2 << at, 3 << at]))
                at += 2
            else:
                stages.append((axis, [1 << at]))
                at += 1
    for axis, masks in stages:
        message = combine([message] + [xor_permute(message, axis, mask) for mask in masks], count)
        count *= len(masks) + 1
    return message, count


def body(scenario_data, cost_matrix, curvature, upper, multipliers, node_map):
    sc_dev, levels, periods, width = scenario_data.shape
    sections = lax.axis_size("section")
    section = lax.axis_index("section")
    section_arg = section.astype(jnp.int32).reshape(1)
    scenarios = sc_dev * sections * lax.axis_size("scen")
    scale = code_scale(width)
    rows = sc_dev * periods
    half = rows // 2
    plane = pl.BlockSpec((periods, width), lambda i: (0, 0))
    smem = pl.BlockSpec(memory_space=pltpu.SMEM)

    order = [1, 0] + list(range(2, levels))
    own_rows, gathered = {}, {}
    for level in order:
        own = scenario_data[:, level].reshape(rows, width)
        own_rows[level] = own
        got = {0: (own[:half], own[half:])}
        for mask in range(1, sections):
            low = mask & -mask
            high = 1 << (mask.bit_length() - 1)
            got[mask] = (xor_permute(got[mask ^ low][0], "section", low), xor_permute(got[mask ^ high][1], "section", high))
        gathered[level] = got

    own_cost = matmul([own_rows[level] for level in order], cost_matrix, levels)
    own_cost = dict(zip(order, own_cost))

    group_map = node_map[0]
    mine = lax.dynamic_slice_in_dim(group_map, section * sc_dev, sc_dev)
    count_mine = jnp.sum((mine[:, None] == group_map[None, :]).astype(F32), axis=1)
    share = 1.0 / count_mine
    before = jnp.where(section > 0, group_map[jnp.maximum(section * sc_dev - 1, 0)], -1)
    after_at = (section + 1) * sc_dev
    after = jnp.where(section + 1 < sections, group_map[jnp.minimum(after_at, group_map.shape[0] - 1)], -1)
    labels = jnp.concatenate([mine, before[None], after[None]]).astype(jnp.int32)

    returned = {}
    for level in order:
        got = gathered[level]
        pieces = [part for mask in range(1, sections) for part in got[mask]]
        blocks = matmul(pieces, cost_matrix, sections - 1, scale)
        returned[level] = [xor_permute(blocks[mask - 1], "section", mask) for mask in range(1, sections)]

    def node_ends(kept, ins, outs):
        marks, = ins
        head, tail = outs
        first, last = marks[0], marks[sc_dev - 1]
        head[...] = kept[0]
        tail[...] = kept[sc_dev - 1]
        for s in range(1, sc_dev):
            @pl.when(marks[s] == first)
            def _():
                head[...] += kept[s]
        for s in range(sc_dev - 1):
            @pl.when(marks[s] == last)
            def _():
                tail[...] += kept[s]

    decisions, second, head, tail = decide(
        1, section_arg, own_cost[1], returned[1], curvature, upper, multipliers, None, scale,
        extra=node_ends, extra_specs=[plane, plane], extra_shapes=[jax.ShapeDtypeStruct((periods, width), F32)] * 2,
        extra_args=[(smem, labels)])
    from_before = lax.ppermute(tail, "section", [(i, i + 1) for i in range(sections - 1)])
    from_after = lax.ppermute(head, "section", [(i + 1, i) for i in range(sections - 1)])

    def node_kernel(marks, shares, value, tail_ref, head_ref, gap, squares, total):
        for s in range(sc_dev):
            total[marks[s]] = jnp.zeros((periods, width), F32)
        for s in range(sc_dev):
            total[marks[s]] += value[s]

        @pl.when(marks[0] == marks[sc_dev])
        def _():
            total[marks[0]] += tail_ref[...]

        @pl.when(marks[sc_dev - 1] == marks[sc_dev + 1])
        def _():
            total[marks[sc_dev - 1]] += head_ref[...]

        acc = jnp.zeros((periods, LANES), F32)
        for s in range(sc_dev):
            off = value[s] - total[marks[s]] * shares[s]
            gap[s] = off
            acc = acc + lane_sum(off * off)
        squares[...] = acc

    vmem = pl.BlockSpec(memory_space=pltpu.VMEM)
    second_gap, second_squares = pl.pallas_call(
        node_kernel,
        in_specs=[smem, smem, vmem, vmem, vmem],
        out_specs=[vmem, vmem],
        out_shape=[jax.ShapeDtypeStruct((sc_dev, periods, width), F32), jax.ShapeDtypeStruct((periods, LANES), F32)],
        scratch_shapes=[pltpu.VMEM((group_map.shape[0], periods, width), F32)],
        cost_estimate=pl.CostEstimate(flops=4000000, bytes_accessed=4000000, transcendentals=0),
    )(labels, share, second, from_before, from_after)

    def first_message(kept, ins, outs):
        squares, = ins
        message, = outs
        total = kept[0]
        for s in range(1, sc_dev):
            total = total + kept[s]
        mean = total * (1.0 / sc_dev)
        acc = squares[...]
        for s in range(sc_dev):
            off = kept[s] - mean
            acc = acc + lane_sum(off * off)
        message[:, :width] = total
        message[:, width:] = acc

    decisions, first, message = decide(
        0, section_arg, own_cost[0], returned[0], curvature, upper, multipliers, decisions, scale,
        extra=first_message, extra_specs=[pl.BlockSpec((periods, width + LANES), lambda i: (0, 0))],
        extra_shapes=[jax.ShapeDtypeStruct((periods, width + LANES), F32)],
        extra_args=[(pl.BlockSpec((periods, LANES), lambda i: (0, 0)), second_squares)])
    message, _ = root_reduce(message, sc_dev)

    for level in order[2:]:
        decisions, = decide(level, section_arg, own_cost[level], returned[level], curvature, upper, multipliers, decisions, scale, keep=False)

    spread = jnp.sum(message[:, width:])
    step = (0.5 / jnp.sqrt(spread / (2.0 * scenarios * periods * width) + 1e-06)).reshape(1)

    def last_kernel(step_ref, mul, first_ref, gap_ref, message_ref, out):
        size = step_ref[0]
        mean = message_ref[:, :width] * (1.0 / scenarios)
        out[:, 0] = mul[:, 0] + size * (first_ref[...] - mean)
        out[:, 1] = mul[:, 1] + size * gap_ref[...]

    part = max(sc_dev // 4, 1)
    new_multipliers = pl.pallas_call(
        last_kernel,
        grid=(sc_dev // part,),
        in_specs=[smem, pl.BlockSpec((part, 2, periods, width), lambda i: (i, 0, 0, 0)), pl.BlockSpec((part, periods, width), lambda i: (i, 0, 0)),
                  pl.BlockSpec((part, periods, width), lambda i: (i, 0, 0)), pl.BlockSpec((periods, width + LANES), lambda i: (0, 0))],
        out_specs=pl.BlockSpec((part, 2, periods, width), lambda i: (i, 0, 0, 0)),
        out_shape=jax.ShapeDtypeStruct(multipliers.shape, F32),
        cost_estimate=pl.CostEstimate(flops=4000000, bytes_accessed=6000000, transcendentals=0),
    )(step, multipliers, first, second_gap, message)
    return new_multipliers, decisions


def solution(mesh):
    by_both = P(("scen", "section"), None, None, None)
    return jax.shard_map(
        body,
        mesh=mesh,
        in_specs=(by_both, P("section", None), by_both, by_both, by_both, P("scen", None)),
        out_specs=(by_both, by_both),
        check_vma=False,
    )
```
